32 devices in a mesh: pair: 16 (over z, y, x), rows: 2 (over core).
Axes of the slice: x: 2, y: 2, z: 4, core: 2. Of those that a mesh axis runs over, the one named last changes fastest.
Arguments:
- samples: float32 [4096, 4096], P(('pair', 'rows')), may hold values from -400 to 400
- keep_mask: int32 [32, 8], P(('pair', 'rows')), may hold values 0 or 1
- keep_rate: float32 [8], replicated, may hold values from 0.5 to 1
Outputs:
- cosine: float32 [64, 512, 512], P('pair', 'rows')
The draws below stay inside these ranges and needn't reach their ends.
All inputs are finite; a program needn't handle non-finite values. No bound on the sum of `keep_mask` on one device may be relied on, other than what follows from the above.
Results may differ from the reference program's by a relative error of at most 0.00005.
Values sent between devices are 32-bit elements; how exact they have to be, the bound alone decides.
No kernel may reach another device: no remote copies, remote signals or barrier semaphores. Data moves between devices by JAX's collectives and lax.ppermute only.
A program may use at most 128 MiB of HBM per device.

```python
import math
import jax
import jax.numpy as jnp
from jax import lax

BLOCKS = 8
BLOCK_COLS = 512
BLOCK_ROWS = 128
COLS = 4096
ROWS_ALL = 4096
ROW_BLOCKS = 32
TILES = 64


def draw_samples(key, part):
    key_noise = jax.random.fold_in(key, 11)
    key_scale = jax.random.fold_in(key, 12)
    noise = jnp.clip(jax.random.normal(key_noise, (ROWS_ALL, COLS + 1), jnp.float32), -6.0, 6.0)
    mixed = noise[:, :COLS] + 0.6 * noise[:, 1:]
    position = jnp.arange(ROWS_ALL, dtype=jnp.float32) / ROWS_ALL
    rising = jnp.exp(jnp.log(3.0) * position)
    factor = jnp.exp(jax.random.uniform(key_scale, (ROWS_ALL,), jnp.float32, jnp.log(0.5), jnp.log(2.0)))
    return (mixed * (factor * rising)[:, None]).astype(jnp.float32)


def with_ends(array, own_key, least, high):
    spot = [jax.random.randint(jax.random.fold_in(own_key, axis), (), 0, length) for axis, length in enumerate(array.shape)]
    longest = array.shape.index(max(array.shape))
    next_to = spot[:longest] + [(spot[longest] + 1) % array.shape[longest]] + spot[longest + 1:]
    return array.at[tuple(spot)].set(least).at[tuple(next_to)].set(high)


def setup_inputs(seed: int = 0) -> dict:
    streams_of = jax.random.split(jax.random.key(seed), 4)
    samples = draw_samples(jax.random.fold_in(streams_of[3], 71), 0)
    keep_mask = with_ends((jax.random.randint(streams_of[1], (ROW_BLOCKS, BLOCKS), 0, 4) < 3).astype(jnp.int32), jax.random.fold_in(streams_of[1], 1), 0, 1)
    keep_rate = jnp.clip(jnp.exp(jax.random.uniform(streams_of[2], (BLOCKS,), jnp.float32, math.log(0.5), math.log(1.0))), 0.5, 1.0)
    return dict(samples=samples, keep_mask=keep_mask, keep_rate=keep_rate)


EPS = 1e-06

def reference(samples, keep_mask, keep_rate):
    weights = keep_mask.astype(jnp.float32)
    masked = samples.reshape(ROW_BLOCKS, BLOCK_ROWS, BLOCKS, BLOCK_COLS) * weights[:, None, :, None]
    masked = masked.reshape(ROWS_ALL, COLS)
    col_norms = jnp.sqrt(lax.optimization_barrier(jnp.sum(samples * samples, axis=0)) + EPS)
    gram = jnp.dot(masked.T, masked, precision=lax.Precision.HIGHEST, preferred_element_type=jnp.float32)
    scale = jnp.repeat(keep_rate, BLOCK_COLS) * col_norms
    cosine = gram / (scale[:, None] * scale[None, :])
    cosine = cosine.reshape(BLOCKS, BLOCK_COLS, BLOCKS, BLOCK_COLS).transpose(0, 2, 1, 3)
    return cosine.reshape(TILES, BLOCK_COLS, BLOCK_COLS)
```

```python
import jax
import jax.numpy as jnp
from jax import lax
from jax.sharding import PartitionSpec as P

BLOCKS = 8
BLOCK_COLS = 512
BLOCK_ROWS = 128


EPS = 1e-06


def plain(samples, keep_mask, keep_rate):
    pair_count = lax.axis_size("pair")
    row_count = lax.axis_size("rows")
    tile_count = BLOCKS * BLOCKS // pair_count
    pair_index = lax.axis_index("pair")
    row_index = lax.axis_index("rows")
    local_rows = samples.shape[0]
    slice_rows = BLOCK_COLS // row_count
    squares = jnp.sum(samples * samples, axis=0)
    col_norms = jnp.sqrt(lax.psum(squares, ("pair", "rows")) + EPS)
    weights = keep_mask.astype(jnp.float32)
    masked = (
        samples.reshape(local_rows // BLOCK_ROWS, BLOCK_ROWS, BLOCKS, BLOCK_COLS)
        * weights[:, None, :, None]
    )
    masked_t = masked.reshape(local_rows, BLOCKS, BLOCK_COLS).transpose(1, 0, 2)
    left_parts = jnp.repeat(masked_t, BLOCKS // tile_count, axis=0)
    right_group = masked_t.reshape(BLOCKS // tile_count, tile_count, local_rows, BLOCK_COLS)
    right_parts = jnp.tile(right_group, (BLOCKS, 1, 1, 1))
    outgoing = jnp.concatenate([left_parts[:, None], right_parts], axis=1)
    received = lax.all_to_all(outgoing, "pair", split_axis=0, concat_axis=0, tiled=True)
    partial_value = jnp.einsum(
        "src,smrd->mcd",
        received[:, 0],
        received[:, 1:],
        precision=lax.Precision.HIGHEST,
        preferred_element_type=jnp.float32,
    )
    summed = lax.psum_scatter(partial_value, "rows", scatter_dimension=1, tiled=True)
    first_tile = pair_index * tile_count
    left_block = first_tile // BLOCKS
    right_start = first_tile % BLOCKS
    norm_blocks = col_norms.reshape(BLOCKS, BLOCK_COLS)
    row_norms = lax.dynamic_slice(
        norm_blocks, (left_block, row_index * slice_rows), (1, slice_rows)
    )[0]
    col_part = lax.dynamic_slice(norm_blocks, (right_start, jnp.int32(0)), (tile_count, BLOCK_COLS))
    left_rate = lax.dynamic_slice(keep_rate, (left_block,), (1,))
    right_rate = lax.dynamic_slice(keep_rate, (right_start,), (tile_count,))
    row_scale = left_rate * row_norms
    col_scale = right_rate[:, None] * col_part
    return summed / (row_scale[None, :, None] * col_scale[:, None, :])


def staged(samples, keep_mask, keep_rate):
    pair_count = lax.axis_size("pair")
    row_count = lax.axis_size("rows")
    tile_count = BLOCKS * BLOCKS // pair_count
    halves = BLOCKS // tile_count
    groups = BLOCKS // 2
    pair_index = lax.axis_index("pair")
    row_index = lax.axis_index("rows")
    local_rows = samples.shape[0]
    slice_rows = BLOCK_COLS // row_count
    half = pair_index % halves
    left_block = pair_index // halves
    group = left_block % groups
    top = left_block // groups

    def swap(value, mask):
        return lax.ppermute(value, "pair", [(p, p ^ mask) for p in range(pair_count)])

    def swap_half(value):
        return swap(value, 1)

    def swap_y(value):
        return swap(value, halves)

    def swap_z(value):
        return swap(value, halves * 2)

    def swap_top(value):
        return swap(value, halves * groups)

    def swap_core(value):
        return lax.ppermute(value, "rows", [(r, r ^ 1) for r in range(row_count)])

    weights = jnp.repeat(keep_mask.astype(jnp.float32), BLOCK_ROWS, axis=0)

    def chunk(k):
        parts = []
        for j in range(2):
            block = (half ^ j) * groups + (group ^ k)
            part = lax.dynamic_slice(samples, (0, block * BLOCK_COLS), (local_rows, BLOCK_COLS))
            parts.append(part * lax.dynamic_slice(weights, (0, block), (local_rows, 1)))
        return jnp.stack(parts)

    def after(value, *others):
        return lax.optimization_barrier((value,) + others)[0]

    own = [chunk(k) for k in range(groups)]
    by_y, by_z, by_d = [None] * 4, [None] * 4, [None] * 4
    by_y[0] = swap_y(own[1])
    by_z[1] = swap_z(own[3])
    by_z[0] = swap_z(own[2])
    by_d[0] = swap_y(by_z[1])
    by_y[1] = swap_y(after(own[0], by_z[1]))
    by_z[2] = swap_z(after(own[0], by_y[0]))
    by_d[1] = swap_y(by_z[0])
    by_y[2] = swap_y(after(own[3], by_z[0]))
    by_d[2] = swap_z(after(by_y[0], by_d[0]))
    by_z[3] = swap_z(after(own[1], by_d[0]))
    by_y[3] = swap_y(after(own[2], by_y[1]))
    by_d[3] = swap_y(by_z[2])

    squares = jnp.sum(samples * samples, axis=0).reshape(BLOCKS, BLOCK_COLS)
    squares = squares + swap_core(squares)
    for mask in (1, halves, halves * 2, halves * groups):
        squares = squares + swap(squares, mask)
    scale = keep_rate[:, None] * jnp.sqrt(squares + EPS)
    row_scale = lax.dynamic_slice(scale, (left_block, row_index * slice_rows), (1, slice_rows))[0]

    out = jnp.zeros((tile_count, slice_rows, BLOCK_COLS), jnp.float32)
    left = None
    for k in range(groups):
        mine = [own[k], by_y[k], by_z[k], by_d[k]]
        rows = jnp.concatenate(mine + [swap_core(part) for part in mine], axis=1)
        if left is None:
            left = jnp.stack([
                lax.dynamic_slice(
                    rows, (half ^ top ^ i, 0, row_index * slice_rows), (1, rows.shape[1], slice_rows)
                )[0]
                for i in range(2)
            ])

        def product(right):
            return jnp.einsum(
                "irm,rn->imn", left, right,
                precision=lax.Precision.HIGH, preferred_element_type=jnp.float32,
            )

        given = swap_half(product(rows[1]))
        summed = product(rows[0]) + given
        total = summed[0] + swap_top(summed[1])
        tile = group ^ k
        col_scale = lax.dynamic_slice(scale, (half * groups + tile, 0), (1, BLOCK_COLS))
        out = lax.dynamic_update_slice(
            out, (total / (row_scale[:, None] * col_scale))[None], (tile, 0, 0)
        )
    return out


def solution(mesh):
    pair_count, row_count = mesh.shape["pair"], mesh.shape["rows"]
    fits = row_count == 2 and pair_count == 2 * BLOCKS
    return jax.shard_map(
        staged if fits else plain,
        mesh=mesh,
        in_specs=(P(("pair", "rows"), None), P(("pair", "rows"), None), P()),
        out_specs=P("pair", "rows", None),
        check_vma=False,
    )
```

```python
import jax
import jax.numpy as jnp
from jax import lax
from jax.sharding import PartitionSpec as P

BLOCKS = 8
BLOCK_COLS = 512
BLOCK_ROWS = 128


EPS = 1e-06


def plain(samples, keep_mask, keep_rate):
    pair_count = lax.axis_size("pair")
    row_count = lax.axis_size("rows")
    tile_count = BLOCKS * BLOCKS // pair_count
    pair_index = lax.axis_index("pair")
    row_index = lax.axis_index("rows")
    local_rows = samples.shape[0]
    slice_rows = BLOCK_COLS // row_count
    squares = jnp.sum(samples * samples, axis=0)
    col_norms = jnp.sqrt(lax.psum(squares, ("pair", "rows")) + EPS)
    weights = keep_mask.astype(jnp.float32)
    masked = (
        samples.reshape(local_rows // BLOCK_ROWS, BLOCK_ROWS, BLOCKS, BLOCK_COLS)
        * weights[:, None, :, None]
    )
    masked_t = masked.reshape(local_rows, BLOCKS, BLOCK_COLS).transpose(1, 0, 2)
    left_parts = jnp.repeat(masked_t, BLOCKS // tile_count, axis=0)
    right_group = masked_t.reshape(BLOCKS // tile_count, tile_count, local_rows, BLOCK_COLS)
    right_parts = jnp.tile(right_group, (BLOCKS, 1, 1, 1))
    outgoing = jnp.concatenate([left_parts[:, None], right_parts], axis=1)
    received = lax.all_to_all(outgoing, "pair", split_axis=0, concat_axis=0, tiled=True)
    partial_value = jnp.einsum(
        "src,smrd->mcd",
        received[:, 0],
        received[:, 1:],
        precision=lax.Precision.HIGHEST,
        preferred_element_type=jnp.float32,
    )
    summed = lax.psum_scatter(partial_value, "rows", scatter_dimension=1, tiled=True)
    first_tile = pair_index * tile_count
    left_block = first_tile // BLOCKS
    right_start = first_tile % BLOCKS
    norm_blocks = col_norms.reshape(BLOCKS, BLOCK_COLS)
    row_norms = lax.dynamic_slice(
        norm_blocks, (left_block, row_index * slice_rows), (1, slice_rows)
    )[0]
    col_part = lax.dynamic_slice(norm_blocks, (right_start, jnp.int32(0)), (tile_count, BLOCK_COLS))
    left_rate = lax.dynamic_slice(keep_rate, (left_block,), (1,))
    right_rate = lax.dynamic_slice(keep_rate, (right_start,), (tile_count,))
    row_scale = left_rate * row_norms
    col_scale = right_rate[:, None] * col_part
    return summed / (row_scale[None, :, None] * col_scale[:, None, :])


def staged(samples, keep_mask, keep_rate):
    pair_count = lax.axis_size("pair")
    row_count = lax.axis_size("rows")
    tile_count = BLOCKS * BLOCKS // pair_count
    halves = BLOCKS // tile_count
    groups = BLOCKS // 2
    pair_index = lax.axis_index("pair")
    row_index = lax.axis_index("rows")
    local_rows = samples.shape[0]
    slice_rows = BLOCK_COLS // row_count
    half = pair_index % halves
    left_block = pair_index // halves
    group = left_block % groups
    top = left_block // groups
    by_half, by_y, by_z, by_top = 1, halves, halves * 2, halves * groups

    def swap(value, mask, name):
        with jax.named_scope(name):
            return lax.ppermute(value, "pair", [(p, p ^ mask) for p in range(pair_count)])

    def swap_core(value, name):
        with jax.named_scope(name):
            return lax.ppermute(value, "rows", [(r, r ^ 1) for r in range(row_count)])

    def after(token, *values):
        gated = lax.optimization_barrier((token,) + values)[1:]
        return gated[0] if len(values) == 1 else gated

    weights = keep_mask.astype(jnp.float32)

    def chunk(k):
        parts = []
        for j in range(2):
            block = (half ^ j) * groups + (group ^ k)
            part = lax.dynamic_slice(samples, (0, block * BLOCK_COLS), (local_rows, BLOCK_COLS))
            weight = lax.dynamic_slice(weights, (0, block), (weights.shape[0], 1))
            parts.append((part.reshape(-1, BLOCK_ROWS, BLOCK_COLS) * weight[:, :, None]).reshape(part.shape))
        return jnp.stack(parts)

    def product(a, b):
        return jnp.einsum(
            "rm,rn->mn", a, b, precision=lax.Precision.HIGH, preferred_element_type=jnp.float32
        )

    own = [None] * groups
    for k in (3, 1, 2, 0):
        own[k] = chunk(k)
    y, z, d = [None] * groups, [None] * groups, [None] * groups
    z[1] = swap(own[3], by_z, "z1")
    y[0] = swap(own[1], by_y, "y0")
    z[0] = swap(own[2], by_z, "z0")
    c0 = swap_core(own[0], "c0")

    d[0] = swap(z[1], by_y, "d0")
    first = after(z[1], own[0])
    y[1] = swap(first, by_y, "y1")
    z[2] = swap(first, by_z, "z2")
    cy0 = swap_core(y[0], "cy0")

    d[1] = swap(z[0], by_y, "d1")
    y[2] = swap(after(z[0], own[3]), by_y, "y2")
    d[2] = swap(after(z[0], y[0]), by_z, "d2")
    z[3] = swap(after(z[0], own[1]), by_z, "z3")
    cz0 = swap_core(z[0], "cz0")
    cd0 = swap_core(d[0], "cd0")

    given = [[None, None] for _ in range(groups)]
    kept = [[None, None] for _ in range(groups)]
    moved, met = [None] * groups, [None] * groups

    def multiply(k, rows):
        second = product(left[1], rows[1])
        given[k][1] = swap(second, by_half, "x%d1" % k)
        first = product(after(second, left[0]), rows[1])
        given[k][0] = swap(first, by_half, "x%d0" % k)
        gated = after(first, left[1], left[0], rows[0])
        kept[k][1] = product(gated[0], gated[2])
        kept[k][0] = product(gated[1], gated[2])
        return first

    def hand_up(k):
        met[k] = kept[k][1] + given[k][1]
        moved[k] = swap(met[k], by_top, "t%d" % k)
        return met[k]

    def gather(k, token):
        mine = list(after(token, own[k], z[k], y[k], d[k]))
        theirs = [swap_core(part, "c%s%d" % (name, k)) for part, name in zip(mine, "ozyd")]
        return jnp.concatenate(mine + theirs, axis=1)

    rows = jnp.concatenate([own[0], z[0], y[0], d[0], c0, cz0, cy0, cd0], axis=1)
    left = [
        lax.dynamic_slice(
            rows, (half ^ top ^ i, 0, row_index * slice_rows), (1, rows.shape[1], slice_rows)
        )[0]
        for i in range(2)
    ]
    token = multiply(0, rows)
    squares = jnp.sum(jnp.square(after(z[1], samples)), axis=0).reshape(BLOCKS, BLOCK_COLS)
    other = swap_core(squares, "s0")
    squares, other = after(token, squares, other)
    squares = squares + other
    other = swap(squares, by_half, "s1")
    y[3] = swap(after(token, own[2], y[1])[0], by_y, "y3")
    d[3] = swap(after(token, z[2]), by_y, "d3")
    token = hand_up(0)
    token = multiply(1, gather(1, token))
    squares, other = after(token, squares, other)
    squares = squares + other
    other = swap(squares, by_y, "s2")
    token = multiply(2, gather(2, token))
    squares, other = after(token, squares, other)
    squares = squares + other
    other = swap(squares, by_z, "s3")
    given[1][1] = after(token, given[1][1])
    token = hand_up(1)
    token = multiply(3, gather(3, token))
    squares, other = after(token, squares, other)
    squares = squares + other
    squares = squares + swap(squares, by_top, "s4")
    given[2][1] = after(token, given[2][1])
    hand_up(2)
    hand_up(3)

    scale = keep_rate[:, None] * jnp.sqrt(squares + EPS)
    row_scale = lax.dynamic_slice(scale, (left_block, row_index * slice_rows), (1, slice_rows))[0]
    out = jnp.zeros((tile_count, slice_rows, BLOCK_COLS), jnp.float32)
    for k in range(groups):
        total = kept[k][0] + given[k][0] + moved[k]
        tile = group ^ k
        col_scale = lax.dynamic_slice(scale, (half * groups + tile, 0), (1, BLOCK_COLS))
        out = lax.dynamic_update_slice(
            out, (total / (row_scale[:, None] * col_scale))[None], (tile, 0, 0)
        )
    return out


def solution(mesh):
    pair_count, row_count = mesh.shape["pair"], mesh.shape["rows"]
    fits = row_count == 2 and pair_count == 2 * BLOCKS
    return jax.shard_map(
        staged if fits else plain,
        mesh=mesh,
        in_specs=(P(("pair", "rows"), None), P(("pair", "rows"), None), P()),
        out_specs=P("pair", "rows", None),
        check_vma=False,
    )
```
